16 devices in a mesh: dp: 4 (over y, z, core), sp: 4 (over x).
Axes of the slice: x: 4, y: 2, z: 1, core: 2. Of those that a mesh axis runs over, the one named last changes fastest.
The devices are a block of a 4x4x8 slice.
Arguments:
- x: bfloat16 [16384, 4096], P(('dp', 'sp')), parts along dimension 0
- gain: bfloat16 [4096], replicated
- wq: bfloat16 [4096, 4096], P('sp')
- wk: bfloat16 [4096, 4096], P('sp')
- wv: bfloat16 [4096, 4096], P('sp')
- wo: bfloat16 [4096, 4096], P('sp')
Outputs:
- output: bfloat16 [16384, 4096], P(('dp', 'sp')), parts along dimension 0
There are 4 independent parts. The reference program is written for one: setup_inputs(seed, part) draws one part's arguments, and reference() takes and returns one part's arrays. A program takes and returns all parts, laid end to end along the dimension named above; an argument that names none is the same for every part.
All inputs are finite; a program needn't handle non-finite values.
Results may differ from the reference program's by a relative error of at most 0.012.
Values are sent between devices in bfloat16 or wider.
A program may use at most 768 MiB of HBM per device.

```python
import jax
import jax.numpy as jnp
from jax import lax

ROWS = 4096
D = 4096
HEADS = 16
KV_HEADS = 16
HEAD = 256
THETA = 10000


def setup_inputs(seed: int = 0, part: int = 0) -> dict:
    kx, kn, kq, kk, kv, ko = jax.random.split(jax.random.key(seed), 6)

    def weights(key, rows, columns):
        return jax.random.normal(key, (rows, columns), jnp.float32) * rows**-0.5

    drawn = {
        "x": jax.random.normal(jax.random.fold_in(kx, part), (ROWS, D), jnp.float32),
        "gain": 1 + 0.1 * jax.random.normal(kn, (D,), jnp.float32),
        "wq": 2 * weights(kq, D, HEADS * HEAD),
        "wk": 2 * weights(kk, D, KV_HEADS * HEAD),
        "wv": 4 * weights(kv, D, KV_HEADS * HEAD),
        "wo": weights(ko, HEADS * HEAD, D),
    }
    return {k: v.astype(jnp.bfloat16) for k, v in drawn.items()}


def normed(x, gain):
    wide = x.astype(jnp.float32)
    scale = lax.rsqrt(jnp.mean(wide * wide, -1, keepdims=True) + 1e-6)
    return (wide * scale * gain.astype(jnp.float32)).astype(jnp.bfloat16)


def turned(t, place, theta):
    half = t.shape[-1] // 2
    angle = place.astype(jnp.float32)[:, None] * theta ** (-jnp.arange(half, dtype=jnp.float32) / half)
    cos, sin = jnp.cos(angle)[:, None], jnp.sin(angle)[:, None]
    a, b = t[..., :half].astype(jnp.float32), t[..., half:].astype(jnp.float32)
    return jnp.concatenate([a * cos - b * sin, b * cos + a * sin], -1).astype(jnp.bfloat16)


def matmul(a, w):
    return jnp.dot(a, w, preferred_element_type=jnp.float32).astype(jnp.bfloat16)


def einsum(form, a, b):
    return jnp.einsum(form, a.astype(jnp.float32), b.astype(jnp.float32))


def attention(q, k, v):
    scores = einsum("tgsd,ugd->gstu", q, k) * q.shape[-1] ** -0.5
    token = jnp.arange(q.shape[0])
    scores = jnp.where(token[:, None] >= token, scores, -jnp.inf)
    weights = jax.nn.softmax(scores, -1).astype(jnp.bfloat16)
    return einsum("gstu,ugd->tgsd", weights, v).astype(jnp.bfloat16)


def reference(x, gain, wq, wk, wv, wo):
    a, place = normed(x, gain), jnp.arange(ROWS)
    q = turned(matmul(a, wq).reshape(ROWS, HEADS, HEAD), place, THETA).reshape(ROWS, KV_HEADS, -1, HEAD)
    k = turned(matmul(a, wk).reshape(ROWS, KV_HEADS, HEAD), place, THETA)
    v = matmul(a, wv).reshape(ROWS, KV_HEADS, HEAD)
    seen = attention(q, k, v).reshape(ROWS, HEADS * HEAD)
    return (x.astype(jnp.float32) + jnp.dot(seen, wo, preferred_element_type=jnp.float32)).astype(jnp.bfloat16)
```

```python
import functools

import jax
import jax.numpy as jnp
from jax import lax
from jax.experimental import pallas as pl
from jax.experimental.pallas import tpu as pltpu
from jax.sharding import PartitionSpec as P


HEAD = 256
THETA = 10000
NEG = -1e30
HIDDEN = 2 * NEG
LOG2E = 1.4426950408889634
VMEM = 56 * 2**20


def _dot(a, b, ca, cb):
    return lax.dot_general(a, b, (((ca,), (cb,)), ((), ())), preferred_element_type=jnp.float32)


TILE = 512


def _attend(q_ref, k_ref, v_ref, o_ref, top_s, mix_s, *, scale):
    heads, bq, d = q_ref.shape
    e = scale * LOG2E
    first = (pl.num_programs(0) - 1 - pl.program_id(0)) * (bq // TILE)
    strips = [(i, at) for at in range(0, bq, TILE) for i in range(heads)]
    top_s[...] = jnp.full(top_s.shape, NEG, jnp.float32)
    mix_s[...] = jnp.zeros(mix_s.shape, jnp.float32)
    ones = jnp.ones((8, TILE), k_ref.dtype)
    seen = lax.broadcasted_iota(jnp.int32, (TILE, TILE), 1) >= lax.broadcasted_iota(jnp.int32, (TILE, TILE), 0)

    def block(j, pieces):
        here = pl.ds(pl.multiple_of(j * TILE, TILE), TILE)
        scores = [_dot(k_ref[i, here, :], q_ref[i, at : at + TILE, :], 1, 1) for i, at, _ in pieces]
        weights, keeps = [], []
        for (i, at, masked), s in zip(pieces, scores):
            if masked:
                s = jnp.where(seen, s, HIDDEN)
            old = top_s[i : i + 1, at : at + TILE]
            top = jnp.maximum(old, s.max(axis=0, keepdims=True))
            top_s[i : i + 1, at : at + TILE] = top
            weights.append(jnp.exp2((s - top) * e).astype(k_ref.dtype))
            keeps.append(jnp.exp2((old - top) * e))
        for (i, at, _), p, keep in zip(pieces, weights, keeps):
            values = jnp.concatenate([v_ref[i, here, :].T, ones], axis=0)
            mix_s[i, :, at : at + TILE] = mix_s[i, :, at : at + TILE] * keep + _dot(values, p, 1, 0)

    lax.fori_loop(0, first, lambda j, _: block(j, [(i, at, False) for i, at in strips]), None)
    for n in range(bq // TILE):
        block(first + n, [(i, at, at == n * TILE) for i, at in strips if at >= n * TILE])
    for i in range(heads):
        total = mix_s[i, d : d + 1, :]
        o_ref[:, i * d : (i + 1) * d] = (mix_s[i, :d, :] * (1 / total)).T.astype(o_ref.dtype)


def attend(kvq, at, count, bq):
    heads, tokens, d = kvq.shape
    n, steps = heads // 3, tokens // bq
    part = lambda base: pl.BlockSpec((count, tokens, d), lambda g: ((base + at) // count, 0, 0))
    return pl.pallas_call(
        functools.partial(_attend, scale=d**-0.5),
        grid=(steps,),
        in_specs=[pl.BlockSpec((count, bq, d), lambda g: ((2 * n + at) // count, steps - 1 - g, 0)), part(0), part(n)],
        out_specs=pl.BlockSpec((bq, count * d), lambda g: (steps - 1 - g, 0)),
        out_shape=jax.ShapeDtypeStruct((tokens, count * d), kvq.dtype),
        scratch_shapes=[pltpu.VMEM((count, bq), jnp.float32), pltpu.VMEM((count, d + 8, bq), jnp.float32)],
        compiler_params=pltpu.CompilerParams(dimension_semantics=("arbitrary",), vmem_limit_bytes=VMEM),
        cost_estimate=pl.CostEstimate(flops=4 * count * tokens * tokens * d, transcendentals=count * tokens * tokens, bytes_accessed=8 * count * tokens * d),
    )(kvq, kvq, kvq)


def _project(pos_ref, *refs, blocks, weights, heads, base):
    given, ws = refs[: 2 * blocks], refs[2 * blocks : 2 * blocks + weights]
    cos_ref, sin_ref = refs[2 * blocks + weights : 2 * blocks + weights + 2]
    o_ref, a_s, sems = refs[-3:]
    b, s = pl.program_id(0), pl.program_id(1)

    def copy(n, k):
        return pltpu.make_async_copy(given[2 * n + k], a_s.at[n % 2], sems.at[n % 2])

    def start(n):
        pl.when(pos_ref[0] == 1)(lambda: copy(n, 0).start())
        pl.when(pos_ref[0] == 0)(lambda: copy(n, 1).start())

    for n in range(blocks):
        @pl.when((b == n) & (s == 0))
        def _():
            if n == 0:
                start(0)
            copy(n, 0).wait()
            if n + 1 < blocks:
                start(n + 1)

    half = HEAD // 2
    for m in range(weights):
        @pl.when((s >= m * heads) & (s < (m + 1) * heads))
        def _():
            t = _dot(a_s[lax.rem(b, 2)], ws[m][...], 1, 0).astype(o_ref.dtype)
            if base // heads + m == 1:
                o_ref[0] = t
            else:
                u, v = t[:, :half].astype(jnp.float32), t[:, half:].astype(jnp.float32)
                cos, sin = cos_ref[...], sin_ref[...]
                o_ref[0, :, :half] = (u * cos - v * sin).astype(o_ref.dtype)
                o_ref[0, :, half:] = (v * cos + u * sin).astype(o_ref.dtype)


def project(home, blocks, ws, base, tables, tokens, buf):
    own, width = blocks[0][0].shape
    heads = ws[0].shape[1] // HEAD
    steps, half = heads * len(ws), HEAD // 2
    anywhere = pl.BlockSpec(memory_space=pl.ANY)
    table = pl.BlockSpec((own, half), lambda b, s, pos: (pos[1 + b], 0))
    specs = [anywhere] * (2 * len(blocks))
    for m in range(len(ws)):
        specs.append(pl.BlockSpec((width, HEAD), lambda b, s, pos, m=m: (0, jnp.clip(s - m * heads, 0, heads - 1))))
    specs += [table, table]
    given = [a for one, other, _ in blocks for a in (one, other)] + [*ws, *tables]
    if buf is not None:
        specs.append(anywhere)
        given.append(buf)
    pos = jnp.stack([jnp.asarray(v, jnp.int32) for v in (home, *[e for _, _, e in blocks])])
    size = own * width * len(blocks)
    return pl.pallas_call(
        functools.partial(_project, blocks=len(blocks), weights=len(ws), heads=heads, base=base),
        grid_spec=pltpu.PrefetchScalarGridSpec(
            num_scalar_prefetch=1,
            grid=(len(blocks), steps),
            in_specs=specs,
            out_specs=pl.BlockSpec((1, own, HEAD), lambda b, s, pos: (base + s, pos[1 + b], 0)),
            scratch_shapes=[pltpu.VMEM((2, own, width), ws[0].dtype), pltpu.SemaphoreType.DMA((2,))],
        ),
        out_shape=jax.ShapeDtypeStruct((3 * heads, tokens, HEAD), ws[0].dtype),
        input_output_aliases={} if buf is None else {len(given): 0},
        compiler_params=pltpu.CompilerParams(dimension_semantics=("arbitrary", "arbitrary"), vmem_limit_bytes=VMEM),
        cost_estimate=pl.CostEstimate(flops=2 * size * steps * HEAD, transcendentals=0, bytes_accessed=2 * size * 2),
    )(pos, *given)


def _mix_most(pos_ref, x_ref, *rest, senders, phases):
    mine = rest[: senders * phases]
    own_ref = rest[senders * phases]
    pieces, (o_ref, last_ref, w_s) = rest[senders * phases + 1 : -3], rest[-3:]
    rows, tile = own_ref.shape
    w_s[pl.ds(pl.multiple_of(pos_ref[0] * rows, rows), rows), :] = own_ref[...]
    for n, piece in enumerate(pieces):
        size = piece.shape[-2]
        w_s[pl.ds(pl.multiple_of(pos_ref[1 + n] * size, size), size), :] = piece[...].reshape(size, tile)
    base = 1 + len(pieces)
    total = x_ref[...].astype(jnp.float32)
    for k in range(senders):
        at = 0
        for p in range(phases):
            m = mine[p * senders + k]
            size = m.shape[1]
            total += _dot(m[...], w_s[pl.ds(pl.multiple_of(pos_ref[base + k] * rows + at, HEAD), size), :], 1, 0)
            at += size
        last = rows - at
        last_ref[k * last : (k + 1) * last, :] = w_s[pl.ds(pl.multiple_of(pos_ref[base + k] * rows + at, HEAD), last), :]
    o_ref[...] = total


def mix_most(pos, x, mine, own, pieces, tile=512):
    tokens, width = x.shape
    rows, senders = own.shape[0], len(mine[0])
    left = rows - sum(m[0].shape[1] for m in mine)
    col = lambda j, pos: (0, j)
    flat = [m for phase in mine for m in phase]
    specs = [pl.BlockSpec((tokens, tile), col)] + [pl.BlockSpec(m.shape, lambda j, pos: (0, 0)) for m in flat] + [pl.BlockSpec((rows, tile), col)]
    for p, _, at in pieces:
        specs.append(pl.BlockSpec((1, p.shape[1], tile), lambda j, pos, at=at: (at, 0, j)))
    return pl.pallas_call(
        functools.partial(_mix_most, senders=senders, phases=len(mine)),
        grid_spec=pltpu.PrefetchScalarGridSpec(
            num_scalar_prefetch=1,
            grid=(width // tile,),
            in_specs=specs,
            out_specs=[pl.BlockSpec((tokens, tile), col), pl.BlockSpec((senders * left, tile), col)],
            scratch_shapes=[pltpu.VMEM((senders * rows, tile), own.dtype)],
        ),
        out_shape=[jax.ShapeDtypeStruct((tokens, width), jnp.float32), jax.ShapeDtypeStruct((senders * left, width), own.dtype)],
        compiler_params=pltpu.CompilerParams(dimension_semantics=("arbitrary",), vmem_limit_bytes=VMEM),
        cost_estimate=pl.CostEstimate(flops=6 * tokens * rows * width, transcendentals=0, bytes_accessed=2 * 4 * rows * width + 6 * tokens * width),
    )(pos, x, *flat, own, *[p for p, _, _ in pieces])


def _mix_last(t_ref, *rest):
    mine, (w_ref, o_ref) = rest[:-2], rest[-2:]
    m = jnp.concatenate([r[...] for r in mine], axis=1)
    o_ref[...] = (t_ref[...] + _dot(m, w_ref[...], 1, 0)).astype(o_ref.dtype)


def mix_last(total, mine, w, tile=512):
    tokens, width = total.shape
    col = lambda j: (0, j)
    return pl.pallas_call(
        _mix_last,
        grid=(width // tile,),
        in_specs=[pl.BlockSpec((tokens, tile), col), *[pl.BlockSpec(m.shape, lambda j: (0, 0)) for m in mine], pl.BlockSpec((w.shape[0], tile), col)],
        out_specs=pl.BlockSpec((tokens, tile), col),
        out_shape=jax.ShapeDtypeStruct((tokens, width), w.dtype),
        compiler_params=pltpu.CompilerParams(dimension_semantics=("arbitrary",), vmem_limit_bytes=VMEM),
        cost_estimate=pl.CostEstimate(flops=2 * tokens * w.shape[0] * width, transcendentals=0, bytes_accessed=6 * tokens * width + 2 * w.size),
    )(total, *mine, w)


def normed(x, gain):
    wide = x.astype(jnp.float32)
    scale = lax.rsqrt(jnp.mean(wide * wide, -1, keepdims=True) + 1e-6)
    return (wide * scale * gain.astype(jnp.float32)).astype(jnp.bfloat16)


def angles(tokens):
    half = HEAD // 2
    angle = jnp.arange(tokens, dtype=jnp.float32)[:, None] * THETA ** (-jnp.arange(half, dtype=jnp.float32) / half)
    return jnp.cos(angle), jnp.sin(angle)


def solution(mesh):
    n, groups = mesh.shape["sp"], mesh.shape["dp"]
    home_at = lambda d, i: (d & 1) == i >> 1

    def move(v, to):
        pairs = [(d * n + i, to(d, i)) for d in range(groups) for i in range(n)]
        pairs = [(a, b[0] * n + b[1]) for a, b in pairs if b is not None]
        return lax.ppermute(v, ("dp", "sp"), pairs)

    across = lambda d, i: (d, i ^ 3)
    beside = lambda d, i: (d, i ^ 1)
    core = lambda d, i: (d ^ 1, i)
    chip = lambda d, i: (d ^ 2, i)
    from_home = lambda to: lambda d, i: to(d, i) if home_at(d, i) else None
    from_away = lambda to: lambda d, i: None if home_at(d, i) else to(d, i)

    def step(x, gain, wq, wk, wv, wo):
      own, _ = x.shape
      i, d = lax.axis_index("sp"), lax.axis_index("dp")
      c, y = d & 1, (d >> 1) & 1
      home = c == (i >> 1)
      rows = wq.shape[0]
      cols = wq.shape[1] // n
      heads = cols // HEAD
      h = (i ^ (i >> 1)) & 1
      mine = 2 * h + c
      theirs = 2 * (1 - h) + c
      part = rows // 2

      def cut(w, g):
          return lax.dynamic_slice(w, (y * part, g * cols), (part, cols))

      pk, ck = move(cut(wk, theirs), beside), move(cut(wk, mine), across)
      pv, pq = move(cut(wv, theirs), beside), move(cut(wq, theirs), beside)
      a = normed(x, gain)
      x1a = move(a, from_home(beside))
      xa = move(a, from_home(core))
      x0 = move(a, from_away(lambda d, i: (d ^ 1, i ^ 3)))
      x1b = move(x0, from_away(beside))
      xc = move(x0, from_away(core))
      xb = move(x1a, from_home(core))
      xd = move(x1b, from_away(core))
      blocks = {"a": (a, xa, i), "b": (x1a, xb, i ^ 1), "c": (xc, x0, i ^ 3), "d": (xd, x1b, i ^ 2)}
      fk = move(pk, across)
      cv, fv = move(cut(wv, mine), across), move(pv, across)
      cq, fq = move(cut(wq, mine), across), move(pq, across)
      full = []
      for w, p, cc, f in ((wk, pk, ck, fk), (wv, pv, cv, fv), (wq, pq, cq, fq)):
          out = jnp.zeros((n * rows, cols), w.dtype)
          out = lax.dynamic_update_slice(out, lax.dynamic_slice(w, (0, mine * cols), (rows, cols)), (i * rows, 0))
          for source, near in ((i ^ 1, p), (i ^ 3, cc), (i ^ 2, f)):
              far = move(near, chip)
              out = lax.dynamic_update_slice(out, near, (source * rows + y * part, 0))
              out = lax.dynamic_update_slice(out, far, (source * rows + (1 - y) * part, 0))
          full.append(out)
      fullk, fullv, fullq = full
      tables = angles(n * own)

      share = d & 3
      quarter = rows // 4
      piece = lax.dynamic_slice(wo, (share * quarter, 0), (quarter, wo.shape[1]))
      oc = move(piece, across)
      op = move(piece, beside)
      ofp = move(oc[quarter // 2 :], beside)
      ofc = move(op[: quarter // 2], across)
      of = jnp.concatenate([ofc, ofp])
      pieces = []
      for t, source in ((oc, i ^ 3), (op, i ^ 1), (of, i ^ 2)):
          ty = move(t, chip)
          both = jnp.stack([t, ty])
          tc = move(both, core)
          pieces += [(both, source * 4 + share, 0), (both, source * 4 + (share ^ 2), 1), (tc, source * 4 + (share ^ 1), 0), (tc, source * 4 + (share ^ 3), 1)]

      def go(which, ws, base, kvq):
          return project(home, [blocks[b] for b in which], ws, base, tables, n * own, kvq)

      kvq = go("a", [fullk], 0, None)
      kvq = go("bc", [fullk], 0, kvq)
      kvq = go("abc", [fullv], heads, kvq)
      kvq = go("abc", [fullq], 2 * heads, kvq)
      kvq = go("d", [fullk, fullv, fullq], 0, kvq)

      arrived = []
      for at, count in ((0, 2), (2, 1), (3, 1)):
          s = attend(kvq, at, count, 2 * own)
          got = []
          for k in range(n):
              to = lambda d, i, k=k: (d, i ^ k) if home_at(d, i) else (d ^ 1, i ^ k ^ 2)
              t = lax.dynamic_slice(s, ((i ^ jnp.where(home, k, k ^ 2)) * own, 0), (own, s.shape[1]))
              r = move(t, from_away(to) if k == 0 else to)
              if k == 0:
                  r = jnp.where(home, t, r)
              got.append(r)
          arrived.append(got)
      senders = []
      for k in range(n):
          chip_k = i ^ jnp.where(home, k if k < 2 else k ^ 2, k ^ 2 if k < 2 else k)
          core_k = (chip_k >> 1) ^ (0 if k < 2 else 1) ^ jnp.where(home, 0, 1)
          senders.append(2 * ((chip_k ^ (chip_k >> 1)) & 1) + core_k)
      pos = jnp.stack([jnp.asarray(v, jnp.int32) for v in (i, *[at for _, at, _ in pieces], *senders)])
      total, last = mix_most(pos, x, arrived[:-1], wo, pieces)
      return mix_last(total, arrived[-1], last)

    tokens, across_rows = P(("dp", "sp"), None), P("sp", None)
    return jax.shard_map(
        step,
        mesh=mesh,
        in_specs=(tokens, P(None), across_rows, across_rows, across_rows, across_rows),
        out_specs=tokens,
        check_vma=False,
    )
```

```python
import functools

import jax
import jax.numpy as jnp
from jax import lax
from jax.experimental import pallas as pl
from jax.experimental.pallas import tpu as pltpu
from jax.sharding import PartitionSpec as P


HEAD = 256
THETA = 10000
NEG = -1e30
HIDDEN = 2 * NEG
LOG2E = 1.4426950408889634
VMEM = 56 * 2**20


def _dot(a, b, ca, cb):
    return lax.dot_general(a, b, (((ca,), (cb,)), ((), ())), preferred_element_type=jnp.float32)


TILE = 512


def _attend(pos_ref, q_ref, k_ref, v_ref, *rest, scale):
    outs, (top_s, mix_s, score_s, out_s, sems) = rest[:-5], rest[-5:]
    heads, bq, d = q_ref.shape
    own = outs[0].shape[0]
    e = scale * LOG2E
    head, step = pl.program_id(0), pl.num_programs(1) - 1 - pl.program_id(1)
    first = step * (bq // TILE)
    strips = [(i, at) for at in range(0, bq, TILE) for i in range(heads)]
    number = {p: n for n, p in enumerate(strips)}
    top_s[...] = jnp.full(top_s.shape, NEG, jnp.float32)
    mix_s[...] = jnp.zeros(mix_s.shape, jnp.float32)
    ones = jnp.ones((8, TILE), k_ref.dtype)
    seen = lax.broadcasted_iota(jnp.int32, (TILE, TILE), 1) >= lax.broadcasted_iota(jnp.int32, (TILE, TILE), 0)

    def keys(j):
        return pl.ds(pl.multiple_of(j * TILE, TILE), TILE)

    def score(j, i, at):
        return _dot(k_ref[i, keys(j), :], q_ref[i, at : at + TILE, :], 1, 1)

    def block(j, slot, pieces, following):
        for p in range(max(len(pieces), len(following))):
            if p < len(following):
                score_s[1 - slot, number[following[p]]] = score(j + 1, *following[p])
            if p < len(pieces):
                i, at, masked = pieces[p]
                s = score_s[slot, number[i, at]]
                if masked:
                    s = jnp.where(seen, s, HIDDEN)
                old = top_s[i : i + 1, at : at + TILE]
                top = jnp.maximum(old, s.max(axis=0, keepdims=True))
                top_s[i : i + 1, at : at + TILE] = top
                weights, keep = jnp.exp2((s - top) * e).astype(k_ref.dtype), jnp.exp2((old - top) * e)
                values = jnp.concatenate([v_ref[i, keys(j), :].T, ones], axis=0)
                mix_s[i, :, at : at + TILE] = mix_s[i, :, at : at + TILE] * keep + _dot(values, weights, 1, 0)

    for p in strips:
        score_s[0, number[p]] = score(0, *p)
    everything = [(i, at, False) for i, at in strips]

    def two(h, _):
        block(2 * h, 0, everything, strips)
        block(2 * h + 1, 1, everything, strips)

    lax.fori_loop(0, lax.div(first, 2), two, None)
    for n in range(bq // TILE):
        block(first + n, n % 2, [(i, at, at == n * TILE) for i, at in strips if at >= n * TILE], [(i, at) for i, at in strips if at > n * TILE])
    out_s[head, step] = (mix_s[0, :d, :] * (1 / mix_s[0, d : d + 1, :])).T.astype(out_s.dtype)

    def copy(n, b, k):
        to = outs[k].at[:, pl.ds(pl.multiple_of(n * d, d), d)]
        return pltpu.make_async_copy(out_s.at[n, step, b * own : (b + 1) * own], to, sems.at[n, k])

    for b in range(bq // own):
        for k in range(len(outs)):
            pl.when(pos_ref[step * (bq // own) + b] == k)(lambda b=b, k=k: copy(head, b, k).start())

    @pl.when((step == 0) & (head == pl.num_programs(0) - 1))
    def _():
        for n in range(out_s.shape[0]):
            for k in range(len(outs)):
                copy(n, 0, k).wait()


def attend(kvq, sender, at, count, bq, own):
    heads, tokens, d = kvq.shape
    n, steps = heads // 3, tokens // bq
    part = lambda base: pl.BlockSpec((1, tokens, d), lambda h, g, pos: (base + at + h, 0, 0))
    return pl.pallas_call(
        functools.partial(_attend, scale=d**-0.5),
        grid_spec=pltpu.PrefetchScalarGridSpec(
            num_scalar_prefetch=1,
            grid=(count, steps),
            in_specs=[pl.BlockSpec((1, bq, d), lambda h, g, pos: (2 * n + at + h, steps - 1 - g, 0)), part(0), part(n)],
            out_specs=[pl.BlockSpec(memory_space=pl.ANY)] * (tokens // own),
            scratch_shapes=[
                pltpu.VMEM((1, bq), jnp.float32),
                pltpu.VMEM((1, d + 8, bq), jnp.float32),
                pltpu.VMEM((2, bq // TILE, TILE, TILE), jnp.float32),
                pltpu.VMEM((count, steps, bq, d), kvq.dtype),
                pltpu.SemaphoreType.DMA((count, tokens // own)),
            ],
        ),
        out_shape=[jax.ShapeDtypeStruct((own, count * d), kvq.dtype)] * (tokens // own),
        compiler_params=pltpu.CompilerParams(dimension_semantics=("arbitrary", "arbitrary"), vmem_limit_bytes=VMEM),
        cost_estimate=pl.CostEstimate(flops=4 * count * tokens * tokens * d, transcendentals=count * tokens * tokens, bytes_accessed=8 * count * tokens * d),
    )(sender, kvq, kvq, kvq)


PIECES = 6
CHUNKS = 2


def _project(pos_ref, *refs, blocks, weights, heads, base):
    given, refs = refs[: 2 * blocks], refs[2 * blocks :]
    ws, refs = [refs[m * (PIECES + 1) : (m + 1) * (PIECES + 1)] for m in range(weights)], refs[weights * (PIECES + 1) :]
    cos_ref, sin_ref, o_ref, a_s, w_s, a_sems, w_sems = refs[0], refs[1], *refs[-5:]
    s, b = pl.program_id(0), pl.program_id(1)
    own = a_s.shape[1]
    chunk = own // CHUNKS

    def fetch(at, slot):
        for m in range(weights):
            @pl.when((at >= m * heads) & (at < (m + 1) * heads))
            def _():
                size = ws[m][1].shape[0]
                for n, w in enumerate(ws[m]):
                    column = (pos_ref[1] * heads if n == 0 else 0) + at - m * heads
                    source = w.at[:, pl.ds(pl.multiple_of(column * HEAD, HEAD), HEAD)]
                    here = pl.ds(pl.multiple_of(pos_ref[2 + n] * size, size), w.shape[0])
                    pltpu.make_async_copy(source, w_s.at[slot, here], w_sems.at[slot]).start()

    def part(n, r, k):
        rows = pl.ds(pl.multiple_of(r * chunk, chunk), chunk)
        return pltpu.make_async_copy(given[2 * n + k].at[rows], a_s.at[n, rows], a_sems.at[n, r])

    def bring(n):
        for r in range(CHUNKS):
            pl.when(pos_ref[0] == 1)(lambda: part(n, r, 0).start())
            pl.when(pos_ref[0] == 0)(lambda: part(n, r, 1).start())

    @pl.when((s == 0) & (b == 0))
    def _():
        fetch(s, 0)
        bring(0)

    slot = lax.rem(s, 2)

    @pl.when(b == 0)
    def _():
        pltpu.make_async_copy(w_s.at[slot], w_s.at[slot], w_sems.at[slot]).wait()
        pl.when(s + 1 < pl.num_programs(0))(lambda: fetch(s + 1, 1 - slot))

    for n in range(1, blocks):
        pl.when((s == 0) & (b == n - 1))(lambda n=n: bring(n))

    half, head = HEAD // 2, base + s
    values = (head >= heads) & (head < 2 * heads)

    def put(rows, t):
        @pl.when(values)
        def _():
            o_ref[0, rows] = t

        @pl.when(jnp.logical_not(values))
        def _():
            u, v = t[:, :half].astype(jnp.float32), t[:, half:].astype(jnp.float32)
            cos, sin = cos_ref[rows], sin_ref[rows]
            o_ref[0, rows, :half] = (u * cos - v * sin).astype(o_ref.dtype)
            o_ref[0, rows, half:] = (v * cos + u * sin).astype(o_ref.dtype)

    def some(r, _):
        for n in range(blocks):
            pl.when((s == 0) & (b == n))(lambda n=n: part(n, r, 0).wait())
        rows = pl.ds(pl.multiple_of(r * chunk, chunk), chunk)
        put(rows, _dot(a_s[b, rows], w_s[slot], 1, 0).astype(o_ref.dtype))

    lax.fori_loop(0, CHUNKS, some, None)


def project(home, mine, blocks, ws, base, tables, tokens, buf):
    own, width = blocks[0][0].shape
    rows, part, cols = ws[0][0].shape[0], *ws[0][1][0][0].shape
    heads, half = cols // HEAD, HEAD // 2
    steps = heads * len(ws)
    anywhere = pl.BlockSpec(memory_space=pl.ANY)
    at_b = 2 + PIECES + 1
    table = pl.BlockSpec((own, half), lambda s, b, pos: (pos[at_b + b], 0))
    given = [a for one, other, _ in blocks for a in (one, other)]
    for w, pieces in ws:
        given += [w, *[p for p, _ in pieces]]
    specs = [anywhere] * len(given) + [table, table]
    given += tables
    if buf is not None:
        specs.append(anywhere)
        given.append(buf)
    places = [p for _, p in ws[0][1]]
    pos = jnp.stack([jnp.asarray(v, jnp.int32) for v in (home, mine, (rows // part) * lax.axis_index("sp"), *places, *[e for _, _, e in blocks])])
    size = own * width * len(blocks)
    return pl.pallas_call(
        functools.partial(_project, blocks=len(blocks), weights=len(ws), heads=heads, base=base),
        grid_spec=pltpu.PrefetchScalarGridSpec(
            num_scalar_prefetch=1,
            grid=(steps, len(blocks)),
            in_specs=specs,
            out_specs=pl.BlockSpec((1, own, HEAD), lambda s, b, pos: (base + s, pos[at_b + b], 0)),
            scratch_shapes=[
                pltpu.VMEM((len(blocks), own, width), w.dtype),
                pltpu.VMEM((2, width, HEAD), w.dtype),
                pltpu.SemaphoreType.DMA((len(blocks), CHUNKS)),
                pltpu.SemaphoreType.DMA((2,)),
            ],
        ),
        out_shape=jax.ShapeDtypeStruct((3 * heads, tokens, HEAD), w.dtype),
        input_output_aliases={} if buf is None else {len(given): 0},
        compiler_params=pltpu.CompilerParams(dimension_semantics=("arbitrary", "arbitrary"), vmem_limit_bytes=VMEM),
        cost_estimate=pl.CostEstimate(flops=2 * size * steps * HEAD, transcendentals=0, bytes_accessed=2 * size * 2),
    )(pos, *given)


def _mix(pos_ref, base_ref, *rest, senders, phases, pieces):
    kept, rest = rest[:phases], rest[phases:]
    mine, rest = rest[: senders * phases], rest[senders * phases :]
    ws, (o_ref, m_s, w_s, sems) = rest[: 1 + pieces], rest[1 + pieces :]
    j = pl.program_id(0)
    tile = o_ref.shape[1]
    heads = m_s.shape[1] // HEAD // senders

    def fetch(at, slot):
        for n, w in enumerate(ws):
            for h in range(heads) if n == 0 else (0,):
                row = pos_ref[1 + n] + h if n == 0 else pos_ref[1 + n]
                source = pl.ds(pl.multiple_of((pos_ref[1 + len(ws)] + h) * HEAD, HEAD), HEAD) if n == 0 else slice(None)
                here = pl.ds(pl.multiple_of(row * HEAD, HEAD), HEAD)
                columns = pl.ds(pl.multiple_of(at * tile, tile), tile)
                copy = lambda w=w, source=source, columns=columns, here=here: pltpu.make_async_copy(
                    w.at[source, columns], w_s.at[slot, here], sems.at[slot]
                ).start()
                pl.when(row >= 0)(copy)

    slot = lax.rem(j, 2)

    @pl.when(j == 0)
    def _():
        fetch(j, 0)
        for k in range(senders):
            at = k * heads * HEAD
            for p in range(phases):
                m = mine[p * senders + k][...]
                if k == 0:
                    m = jnp.where(pos_ref[0] == 1, kept[p][...], m)
                m_s[:, at : at + m.shape[1]] = m
                at += m.shape[1]

    pltpu.make_async_copy(w_s.at[slot], w_s.at[slot], sems.at[slot]).wait()
    pl.when(j + 1 < pl.num_programs(0))(lambda: fetch(j + 1, 1 - slot))
    o_ref[...] = (base_ref[...].astype(jnp.float32) + _dot(m_s[...], w_s[slot], 1, 0)).astype(o_ref.dtype)


def mix(pos, base, kept, mine, ws, dtype, tile=512):
    tokens, width = base.shape
    flat = kept + [m for phase in mine for m in phase]
    rows = sum(m.shape[1] for phase in mine for m in phase)
    col = lambda j, pos: (0, j)
    return pl.pallas_call(
        functools.partial(_mix, senders=len(mine[0]), phases=len(mine), pieces=len(ws) - 1),
        grid_spec=pltpu.PrefetchScalarGridSpec(
            num_scalar_prefetch=1,
            grid=(width // tile,),
            in_specs=[pl.BlockSpec((tokens, tile), col), *[pl.BlockSpec(m.shape, lambda j, pos: (0, 0)) for m in flat]]
            + [pl.BlockSpec(memory_space=pl.ANY)] * len(ws),
            out_specs=pl.BlockSpec((tokens, tile), col),
            scratch_shapes=[pltpu.VMEM((tokens, rows), flat[0].dtype), pltpu.VMEM((2, rows, tile), ws[0].dtype), pltpu.SemaphoreType.DMA((2,))],
        ),
        out_shape=jax.ShapeDtypeStruct((tokens, width), dtype),
        compiler_params=pltpu.CompilerParams(dimension_semantics=("arbitrary",), vmem_limit_bytes=VMEM),
        cost_estimate=pl.CostEstimate(flops=2 * tokens * rows * width, transcendentals=0, bytes_accessed=2 * rows * width + 6 * tokens * width),
    )(pos, base, *flat, *ws)


def _norm(x_ref, gain_ref, o_ref):
    wide = x_ref[...].astype(jnp.float32)
    scale = lax.rsqrt(jnp.mean(wide * wide, -1, keepdims=True) + 1e-6)
    o_ref[...] = (wide * scale * gain_ref[...].astype(jnp.float32)).astype(o_ref.dtype)


def normed(x, gain, tile=128):
    tokens, width = x.shape
    return pl.pallas_call(
        _norm,
        grid=(tokens // tile,),
        in_specs=[pl.BlockSpec((tile, width), lambda j: (j, 0)), pl.BlockSpec((1, width), lambda j: (0, 0))],
        out_specs=pl.BlockSpec((tile, width), lambda j: (j, 0)),
        out_shape=jax.ShapeDtypeStruct(x.shape, x.dtype),
        compiler_params=pltpu.CompilerParams(dimension_semantics=("arbitrary",), vmem_limit_bytes=VMEM),
        cost_estimate=pl.CostEstimate(flops=5 * x.size, transcendentals=tokens, bytes_accessed=4 * x.size),
    )(x, gain[None])


def angles(tokens):
    half = HEAD // 2
    angle = jnp.arange(tokens, dtype=jnp.float32)[:, None] * THETA ** (-jnp.arange(half, dtype=jnp.float32) / half)
    return jnp.cos(angle), jnp.sin(angle)


PHASES = ((0, 2), (2, 2))


def solution(mesh):
    n, groups = mesh.shape["sp"], mesh.shape["dp"]
    home_at = lambda d, i: (d & 1) == i >> 1

    def move(v, to):
        pairs = [(d * n + i, to(d, i)) for d in range(groups) for i in range(n)]
        pairs = [(a, b[0] * n + b[1]) for a, b in pairs if b is not None]
        return lax.ppermute(v, ("dp", "sp"), pairs)

    across = lambda d, i: (d, i ^ 3)
    beside = lambda d, i: (d, i ^ 1)
    core = lambda d, i: (d ^ 1, i)
    chip = lambda d, i: (d ^ 2, i)
    from_home = lambda to: lambda d, i: to(d, i) if home_at(d, i) else None
    from_away = lambda to: lambda d, i: None if home_at(d, i) else to(d, i)

    def step(x, gain, wq, wk, wv, wo):
      own, _ = x.shape
      i, d = lax.axis_index("sp"), lax.axis_index("dp")
      c, y = d & 1, (d >> 1) & 1
      home = c == (i >> 1)
      rows = wq.shape[0]
      cols = wq.shape[1] // n
      heads = cols // HEAD
      h = (i ^ (i >> 1)) & 1
      mine = 2 * h + c
      theirs = 2 * (1 - h) + c
      part = rows // 2

      def cut(w, g):
          return lax.dynamic_slice(w, (y * part, g * cols), (part, cols))

      pk, ck = move(cut(wk, theirs), beside), move(cut(wk, mine), across)
      pv, pq = move(cut(wv, theirs), beside), move(cut(wq, theirs), beside)
      a = normed(x, gain)
      x1a = move(a, from_home(beside))
      xa = move(a, from_home(core))
      x0 = move(a, from_away(lambda d, i: (d ^ 1, i ^ 3)))
      x1b = move(x0, from_away(beside))
      xc = move(x0, from_away(core))
      xb = move(x1a, from_home(core))
      xd = move(x1b, from_away(core))
      blocks = {"a": (a, xa, i), "b": (x1a, xb, i ^ 1), "c": (xc, x0, i ^ 3), "d": (xd, x1b, i ^ 2)}
      fk = move(pk, across)
      cv, fv = move(cut(wv, mine), across), move(pv, across)
      cq, fq = move(cut(wq, mine), across), move(pq, across)
      ws = {}
      for name, w, p, cc, f in (("k", wk, pk, ck, fk), ("v", wv, pv, cv, fv), ("q", wq, pq, cq, fq)):
          pieces = []
          for source, near in ((i ^ 1, p), (i ^ 3, cc), (i ^ 2, f)):
              pieces += [(near, 2 * source + y), (move(near, chip), 2 * source + 1 - y)]
          ws[name] = (w, pieces)
      tables = angles(n * own)

      share = d & 3
      quarter = rows // 4
      piece = lax.dynamic_slice(wo, (share * quarter, 0), (quarter, wo.shape[1]))
      oc = move(piece, across)
      op = move(piece, beside)
      of = move(op, across)
      pieces = []
      for t, source in ((oc, i ^ 3), (op, i ^ 1), (of, i ^ 2)):
          ty = move(t, chip)
          pieces += [(t, source * 4 + share), (ty, source * 4 + (share ^ 2))]
          pieces += [(move(t, core), source * 4 + (share ^ 1)), (move(ty, core), source * 4 + (share ^ 3))]

      def go(which, kinds, base, kvq):
          return project(home, mine, [blocks[b] for b in which], [ws[k] for k in kinds], base, tables, n * own, kvq)

      kvq = go("a", "k", 0, None)
      kvq = go("c", "k", 0, kvq)
      kvq = go("b", "k", 0, kvq)
      kvq = go("a", "v", heads, kvq)
      kvq = go("bc", "v", heads, kvq)
      kvq = go("abc", "q", 2 * heads, kvq)
      kvq = go("d", "kvq", 0, kvq)

      sender = jnp.stack([i ^ b ^ jnp.where(home, 0, 2) for b in range(n)]).astype(jnp.int32)
      kept, arrived = [], []
      for at, count in PHASES:
          sent = attend(kvq, sender, at, count, 2 * own, own)
          kept.append(sent[0])
          got = []
          for k in range(n):
              to = lambda d, i, k=k: (d, i ^ k) if home_at(d, i) else (d ^ 1, i ^ k ^ 2)
              got.append(move(sent[k], from_away(to) if k == 0 else to))
          arrived.append(got)
      senders = []
      for k in range(n):
          chip_k = i ^ jnp.where(home, k if k < 2 else k ^ 2, k ^ 2 if k < 2 else k)
          core_k = (chip_k >> 1) ^ (0 if k < 2 else 1) ^ jnp.where(home, 0, 1)
          senders.append(2 * ((chip_k ^ (chip_k >> 1)) & 1) + core_k)

      def placed(shard, quarter, low, high):
          order = sum(k * (senders[k] == shard).astype(jnp.int32) for k in range(n))
          return jnp.where((quarter >= low) & (quarter < high), order * (high - low) + quarter - low, -1)

      split = sum(count for _, count in PHASES[:-1])
      total = x
      for low, high, part, dtype in ((0, split, slice(0, -1), jnp.float32), (split, heads, slice(-1, None), x.dtype)):
          places = [placed(i, jnp.int32(low), low, high), *[placed(at // heads, at % heads, low, high) for _, at in pieces]]
          pos = jnp.stack([jnp.asarray(v, jnp.int32) for v in (home, *places, low)])
          total = mix(pos, total, kept[part], arrived[part], [wo, *[p for p, _ in pieces]], dtype)
      return total

    tokens, across_rows = P(("dp", "sp"), None), P("sp", None)
    return jax.shard_map(
        step,
        mesh=mesh,
        in_specs=(tokens, P(None), across_rows, across_rows, across_rows, across_rows),
        out_specs=tokens,
        check_vma=False,
    )
```
